32 devices in a mesh: task: 2 (over x), ctx: 16 (over z, y, core).
Axes of the slice: x: 2, y: 2, z: 4, core: 2. Of those that a mesh axis runs over, the one named last changes fastest.
Arguments:
- base_queries: bfloat16 [2, 2048, 2048], P('task', 'ctx'), may hold values from -48 to 48
- adapter_input: bfloat16 [2, 2048, 16], P('task', 'ctx'), may hold values from -6 to 6
- adapter_up_weight: bfloat16 [2, 16, 2048], P('task'), may hold values from -1.5 to 1.5
- projected_keys: bfloat16 [2, 2048, 512], P('task', 'ctx'), may hold values from -6 to 6
- projected_values: bfloat16 [2, 2048, 512], P('task', 'ctx'), may hold values from -6 to 6
- output_gradient: bfloat16 [2, 2048, 2048], P('task', 'ctx'), may hold values from -0.52734375 to 0.52734375
- segments: int32 [2, 2048], P('task', 'ctx'), may hold values from 0 to 4, never falling along the last dimension, each value on 1 to 768 neighbouring positions
- solution: float32 [2, 32768], P('task'), may hold values from -1.5 to 1.5
- residual: float32 [2, 32768], P('task'), may hold values from -1.5 to 1.5
- direction: float32 [2, 32768], P('task'), may hold values from -1.5 to 1.5
- damping: float32 [2], P('task'), may hold values from 2 to 8
Outputs:
- new_solution: float32 [2, 32768], P('task', 'ctx')
- new_residual: float32 [2, 32768], P('task', 'ctx')
- new_direction: float32 [2, 32768], P('task', 'ctx')
- meta_gradient: float32 [32768], P('ctx')
The draws below stay inside these ranges and needn't reach their ends.
Inputs may be any that keep to these rules, and one draw needn't show every extreme that they name: `segments`: segment numbers never fall along a task's tokens; each document holds 1 to 768 tokens, and some document holds exactly 768.
All inputs are finite; a program needn't handle non-finite values.
Results may differ from the reference program's by a relative error of at most 0.0073.
Values may be sent and summed in bfloat16 or wider, within the bound.
A program may use at most 64 MiB of HBM per device.

```python
import math
import jax
import jax.numpy as jnp
import numpy as np
from jax import lax

HEADS = 16
KV_HEADS = 4
HEAD_DIM = 128
ADAPTER_RANK = 16
TOKENS_PER_SHARD = 128
TASK_COUNT = 2
TASK_TOKENS = 2048
DOC = 768
DOCS = 5
QUERY_FEATURES = 2048
KW = 512
PARAMS = 32768


def joint_draw(key):
    seeded = jax.random.fold_in(key, 7301)
    query_key, key_key = jax.random.split(seeded, 2)
    key_field = jnp.clip(jax.random.normal(key_key, (TASK_COUNT, TASK_TOKENS, KV_HEADS, HEAD_DIM), jnp.float32), -6.0, 6.0)
    query_field = jnp.clip(jax.random.normal(query_key, (TASK_COUNT, TASK_TOKENS, HEADS, HEAD_DIM), jnp.float32), -6.0, 6.0)
    return (query_field.reshape(TASK_COUNT, TASK_TOKENS, HEADS * HEAD_DIM), key_field.reshape(TASK_COUNT, TASK_TOKENS, KV_HEADS * HEAD_DIM))


def draw_base_queries(key, part):
    return joint_draw(key)[0].astype(jnp.bfloat16)


def draw_projected_keys(key, part):
    return joint_draw(key)[1].astype(jnp.bfloat16)


def level_of(key, dims, shards, low, high):
    factor_of = 1.0
    for axis_at, blocks in shards:
        heights = jax.random.uniform(jax.random.fold_in(jax.random.fold_in(key, 6), axis_at), (blocks,), jnp.float32, low / len(shards), high / len(shards))
        factor_of = factor_of * jnp.repeat(jnp.exp(heights), dims[axis_at] // blocks).reshape((-1,) + (1,) * (len(dims) - 1 - axis_at))
    return factor_of


def length_profile(number_of, total, limit, lean):
    weights = [(1 << 20) // math.isqrt(standing ** lean) + 1 for standing in range(2, number_of + 1)]
    spare, counts = total - limit - (number_of - 1), [1] * (number_of - 1)
    while spare > 0:
        free = [i for i in range(number_of - 1) if counts[i] < limit]
        mass, left = sum([weights[i] for i in free]), spare
        for i in free:
            more = min(limit - counts[i], max(1, left * weights[i] // mass), spare)
            counts[i] = counts[i] + more
            spare = spare - more
    return np.array([limit] + counts)


def ragged(stream_key, amount, total, bound, slope):
    if amount == 2:
        one = jax.random.randint(stream_key, (), max(1, total - bound), min(bound, total - 1) + 1)
        return jnp.stack([one, total - one])
    lengths = jnp.asarray(length_profile(amount, total, bound, slope), jnp.int32)
    pairs = (amount - 1) // 2
    donor, sink = lengths[1:1 + 2 * pairs:2], lengths[2:2 + 2 * pairs:2]
    room = jnp.minimum(donor - 1, bound - sink)
    shifted = jax.random.randint(jax.random.fold_in(stream_key, 1), (pairs,), 0, 1 << 20) % (room + 1)
    lengths = lengths.at[1:1 + 2 * pairs:2].set(donor - shifted).at[2:2 + 2 * pairs:2].set(sink + shifted)
    return lengths[jax.random.permutation(jax.random.fold_in(stream_key, 2), amount)]


def bell_draw(stream_key, dims, spread, limit, cuts=(), kind=jnp.bfloat16):
    array = jax.random.normal(stream_key, dims, jnp.float32) * spread
    if len(cuts) > 0:
        array = level_of(stream_key, dims, cuts, -0.22, 0.18) * array
    return jnp.clip(array, min=-limit, max=limit).astype(kind)


def setup_inputs(seed: int = 0) -> dict:
    arg_keys = jax.random.split(jax.random.key(seed), 12)
    base_queries = draw_base_queries(jax.random.fold_in(arg_keys[11], 71), 0)
    adapter_input = bell_draw(arg_keys[1], (TASK_COUNT, TASK_TOKENS, ADAPTER_RANK), 1.0, 6.0, ((0, 2), (1, 16)))
    adapter_up_weight = bell_draw(arg_keys[2], (TASK_COUNT, ADAPTER_RANK, QUERY_FEATURES), ADAPTER_RANK ** -0.5, 1.5, ((0, 2),))
    projected_keys = draw_projected_keys(jax.random.fold_in(arg_keys[11], 71), 0)
    projected_values = bell_draw(arg_keys[4], (TASK_COUNT, TASK_TOKENS, KW), 1.0, 6.0, ((0, 2), (1, 16)))
    output_gradient = bell_draw(arg_keys[5], (TASK_COUNT, TASK_TOKENS, QUERY_FEATURES), (HEAD_DIM ** -0.5), 0.52734375, ((0, 2), (1, 16)))
    segments = jax.vmap(lambda own: jnp.searchsorted(jnp.cumsum(ragged(own, DOCS, TASK_TOKENS, DOC, 0)), jnp.arange(TASK_TOKENS), side="right"))(jax.random.split(arg_keys[6], TASK_COUNT)).reshape((TASK_COUNT, TASK_TOKENS)).astype(jnp.int32)
    solution = bell_draw(arg_keys[7], (TASK_COUNT, PARAMS), 0.25, 1.5, ((0, 2),), jnp.float32)
    residual = bell_draw(arg_keys[8], (TASK_COUNT, PARAMS), 0.25, 1.5, ((0, 2),), jnp.float32)
    direction = bell_draw(arg_keys[9], (TASK_COUNT, PARAMS), 0.25, 1.5, ((0, 2),), jnp.float32)
    damping = jnp.clip(jnp.exp(math.log(8.0) - 1.3862944 * jax.random.uniform(arg_keys[10], (TASK_COUNT,), jnp.float32) ** level_of(arg_keys[10], (TASK_COUNT,), ((0, 2),), -0.2, 0.2)), 2.0, 8.0)
    return dict(base_queries=base_queries, adapter_input=adapter_input, adapter_up_weight=adapter_up_weight, projected_keys=projected_keys, projected_values=projected_values, output_gradient=output_gradient, segments=segments, solution=solution, residual=residual, direction=direction, damping=damping)


def attend(query_matrix, tangent_vectors, grads_in, key_window, value_window, allowed):
    per_group = HEADS // KV_HEADS
    score_scale = HEAD_DIM ** -0.5
    row_count = query_matrix.shape[0]
    head_parts = []
    for kv_index in range(KV_HEADS):
        low_col = kv_index * per_group * HEAD_DIM
        high_col = low_col + per_group * HEAD_DIM
        query_head = query_matrix[:, low_col:high_col].reshape(row_count, per_group, HEAD_DIM).astype(jnp.float32)
        tangent_head = tangent_vectors[:, low_col:high_col].reshape(row_count, per_group, HEAD_DIM).astype(jnp.float32)
        grad_head = grads_in[:, low_col:high_col].reshape(row_count, per_group, HEAD_DIM).astype(jnp.float32)
        key_head = key_window[:, kv_index * HEAD_DIM:(kv_index + 1) * HEAD_DIM].astype(jnp.float32)
        value_head = value_window[:, kv_index * HEAD_DIM:(kv_index + 1) * HEAD_DIM].astype(jnp.float32)
        scores = jnp.einsum("tgd,kd->tgk", query_head, key_head) * score_scale
        slopes = jnp.einsum("tgd,kd->tgk", tangent_head, key_head) * score_scale
        pulls = jnp.einsum("tgd,kd->tgk", grad_head, value_head)
        key_mask = allowed[:, None, :]
        masked = jnp.where(key_mask, scores, -1e30)
        row_max = jnp.max(masked, axis=2, keepdims=True)
        exp_terms = jnp.exp(masked - row_max)
        probability = exp_terms / jnp.sum(exp_terms, axis=2, keepdims=True)
        mean_slope = jnp.sum(probability * slopes, axis=2, keepdims=True)
        mean_pull = jnp.sum(probability * pulls, axis=2, keepdims=True)
        centred = (slopes - mean_slope) * (pulls - mean_pull)
        covariance = jnp.sum(probability * centred, axis=2, keepdims=True)
        coef_rounded = (probability * (centred - covariance)).astype(jnp.bfloat16)
        coef_back = lax.optimization_barrier(coef_rounded).astype(jnp.float32)
        head_rows = jnp.einsum("tgk,kd->tgd", coef_back, key_head) * score_scale
        head_parts.append(head_rows.reshape(row_count, per_group * HEAD_DIM))
    return jnp.concatenate(head_parts, axis=1)


def task_contribution(base_queries, adapter_input, adapter_up_weight, projected_keys, projected_values, output_gradient, segments, direction):
    query_matrix = (base_queries.astype(jnp.float32) + jnp.dot(adapter_input, adapter_up_weight, preferred_element_type=jnp.float32)).astype(jnp.bfloat16)
    shift_matrix_fn = direction.reshape(ADAPTER_RANK, HEADS * HEAD_DIM)
    tangent_vectors = jnp.dot(adapter_input.astype(jnp.float32), shift_matrix_fn, precision=lax.Precision.HIGHEST).astype(jnp.bfloat16)
    key_width = KV_HEADS * HEAD_DIM
    key_padded = jnp.concatenate([jnp.zeros((DOC, key_width), jnp.bfloat16), projected_keys], axis=0)
    value_padded = jnp.concatenate([jnp.zeros((DOC, key_width), jnp.bfloat16), projected_values], axis=0)
    seg_padded = jnp.concatenate([jnp.zeros((DOC,), jnp.int32), segments.astype(jnp.int32)], axis=0)
    window = DOC + TOKENS_PER_SHARD

    def one_block(block_id):
        leading_row = (block_id * TOKENS_PER_SHARD).astype(jnp.int32)
        query_rows = lax.dynamic_slice_in_dim(query_matrix, leading_row, TOKENS_PER_SHARD, 0)
        tangent_rows = lax.dynamic_slice_in_dim(tangent_vectors, leading_row, TOKENS_PER_SHARD, 0)
        grad_rows = lax.dynamic_slice_in_dim(output_gradient, leading_row, TOKENS_PER_SHARD, 0)
        adapter_rows = lax.dynamic_slice_in_dim(adapter_input, leading_row, TOKENS_PER_SHARD, 0)
        seg_rows = lax.dynamic_slice_in_dim(segments.astype(jnp.int32), leading_row, TOKENS_PER_SHARD, 0)
        key_window = lax.dynamic_slice_in_dim(key_padded, leading_row, window, 0)
        value_window = lax.dynamic_slice_in_dim(value_padded, leading_row, window, 0)
        seg_window = lax.dynamic_slice_in_dim(seg_padded, leading_row, window, 0)
        key_place = leading_row - DOC + jnp.arange(window, dtype=jnp.int32)
        query_place = leading_row + jnp.arange(TOKENS_PER_SHARD, dtype=jnp.int32)
        allowed = (key_place[None, :] <= query_place[:, None]) & (key_place[None, :] >= 0) & (seg_window[None, :] == seg_rows[:, None])
        curvature_product_rows = attend(query_rows, tangent_rows, grad_rows, key_window, value_window, allowed).astype(jnp.bfloat16)
        return jnp.dot(adapter_rows.T, curvature_product_rows, preferred_element_type=jnp.float32)

    block_terms = lax.map(one_block, jnp.arange(TASK_TOKENS // TOKENS_PER_SHARD, dtype=jnp.int32))
    return jnp.sum(block_terms, axis=0).reshape(ADAPTER_RANK * HEADS * HEAD_DIM)


def reference(base_queries, adapter_input, adapter_up_weight, projected_keys, projected_values, output_gradient, segments, solution, residual, direction, damping):
    def task_wise(items):
        return task_contribution(items[0], items[1], items[2], items[3], items[4], items[5], items[6], items[7])

    complete_curvature_product = lax.map(task_wise, (base_queries, adapter_input, adapter_up_weight, projected_keys, projected_values, output_gradient, segments, direction))
    curved = direction + complete_curvature_product / damping[:, None]
    old_norm = jnp.sum(residual * residual, axis=1)
    step_len = old_norm / jnp.sum(direction * curved, axis=1)
    new_solution = solution + step_len[:, None] * direction
    new_residual = residual - step_len[:, None] * curved
    ratio = jnp.sum(new_residual * new_residual, axis=1) / old_norm
    new_direction = new_residual + ratio[:, None] * direction
    meta_gradient = jnp.mean(new_solution, axis=0)
    return new_solution, new_residual, new_direction, meta_gradient
```

```python
import functools

import jax
import jax.numpy as jnp
from jax import lax
from jax.experimental import pallas as pl
from jax.experimental.pallas import tpu as pltpu
from jax.sharding import PartitionSpec as P

KV_HEADS = 4
HEAD_DIM = 128
SPAN = 6
LANES = 128
MESH = pl.DeviceIdType.MESH
NT = (((1,), (1,)), ((), ()))


def kernel(
    dims,
    base_ref, ain_ref, up_ref, key_ref, val_ref, grad_ref, seg_ref,
    sol_ref, res_ref, dir_ref, dirmat_ref, damp_ref,
    nsol_ref, nres_ref, ndir_ref, meta_ref,
    kbuf, vbuf, segbuf, qin, gin, ain, qs, ts, gs, dsel,
    sbuf, tbuf, ubuf, mbuf, cbuf, hvacc, hvsend, hvrecv, dhsend, dhrecv,
    nrsend, nrrecv, solrecv,
    own_send, sib_send, sib_recv, seg_send, seg_recv, k_recv, v_recv, relay_send,
    hv_ssem, hv_rsem, dh_ssem, dh_rsem, nr_ssem, nr_rsem, sol_ssem, sol_rsem,
):
    tasks, ctx, rank, heads, part_rows, piece, nq = dims
    chips = ctx // 2
    per = heads // KV_HEADS
    tok = base_ref.shape[0]
    half = heads * HEAD_DIM // 2
    khalf = key_ref.shape[1] // 2
    hloc = heads // 2
    kvloc = KV_HEADS // 2
    nwin = SPAN + 2
    win = SPAN + 1
    back = SPAN // 2
    wide = per * tok
    f32, bf16 = jnp.float32, jnp.bfloat16
    me_t = lax.axis_index("task")
    me = lax.axis_index("ctx")
    c = me // 2
    k = lax.rem(me, 2)
    odd = lax.rem(c, 2)
    sib = me + 1 - 2 * k

    def dev(n):
        return (me_t, n)

    barrier = pltpu.get_barrier_semaphore()

    def greet(i, carry):
        pl.semaphore_signal(barrier, inc=1, device_id=dev(lax.rem(me + i, ctx)), device_id_type=MESH)
        return carry

    lax.fori_loop(1, ctx, greet, 0)
    for i in range(1, tasks):
        pl.semaphore_signal(barrier, inc=1, device_id=(lax.rem(me_t + i, tasks), me), device_id_type=MESH)
    pl.semaphore_wait(barrier, ctx - 1 + tasks - 1)

    def rc(src, dst, ssem, rsem, n):
        return pltpu.make_async_remote_copy(
            src_ref=src, dst_ref=dst, send_sem=ssem, recv_sem=rsem, device_id=dev(n), device_id_type=MESH
        )

    def kcols(h):
        return pl.ds(pl.multiple_of(h * khalf, LANES), khalf)

    def qcols(h):
        return pl.ds(pl.multiple_of(h * half, LANES), half)

    other = 1 - k
    sib_copies = [
        rc(ain_ref, ain.at[k], sib_send.at[0], sib_recv.at[0], sib),
        rc(base_ref.at[:, qcols(other)], qin.at[k], sib_send.at[1], sib_recv.at[1], sib),
        rc(grad_ref.at[:, qcols(other)], gin.at[k], sib_send.at[2], sib_recv.at[2], sib),
        rc(key_ref.at[:, kcols(other)], kbuf.at[SPAN + k], sib_send.at[3], k_recv.at[SPAN + k], sib),
        rc(val_ref.at[:, kcols(other)], vbuf.at[SPAN + k], sib_send.at[4], v_recv.at[SPAN + k], sib),
    ]
    ahead2, ahead1 = [], []
    for h in range(2):
        for copies, d in ((ahead2, 2), (ahead1, 1)):
            n = 2 * (c + d) + h
            w = SPAN - 2 * d + k
            s = 4 * (d - 1) + 2 * h
            copies.append(rc(key_ref.at[:, kcols(h)], kbuf.at[w], own_send.at[s], k_recv.at[w], n))
            copies.append(rc(val_ref.at[:, kcols(h)], vbuf.at[w], own_send.at[s + 1], v_recv.at[w], n))
    seg_copies = []
    for d in range(back + 1):
        for h in range(2):
            w = SPAN - 2 * d + k
            n = 2 * (c + d) + h
            seg_copies.append((d, h, rc(seg_ref, segbuf.at[w], seg_send.at[2 * d + h], seg_recv.at[w], n)))
    go2 = c + 2 < chips
    go1 = odd == 0

    def start_all(copies):
        for copy in copies:
            copy.start()

    pl.when(go2)(lambda: start_all(ahead2))
    pl.when(go1)(lambda: start_all(ahead1))
    start_all(sib_copies)
    for d, h, copy in seg_copies:
        ok = (c + d < chips) if d else (k != h)
        pl.when(ok)(copy.start)

    for w in range(SPAN):
        @pl.when(c < back - w // 2)
        def _(w=w):
            kbuf[w] = jnp.zeros(kbuf.shape[1:], bf16)
            vbuf[w] = jnp.zeros(vbuf.shape[1:], bf16)
            segbuf[w] = jnp.full(segbuf.shape[1:], -1, jnp.int32)

    for s in range(2):
        @pl.when(k == s)
        def _(s=s):
            kbuf[SPAN + s] = key_ref[:, s * khalf:(s + 1) * khalf]
            vbuf[SPAN + s] = val_ref[:, s * khalf:(s + 1) * khalf]
            segbuf[SPAN + s] = seg_ref[...]
            qin[s] = base_ref[:, s * half:(s + 1) * half]
            gin[s] = grad_ref[:, s * half:(s + 1) * half]
            ain[s] = ain_ref[...]

    first = k == 0
    up = jnp.where(first, up_ref[:, :half].astype(f32), up_ref[:, half:].astype(f32)).astype(bf16)
    for j in range(hloc):
        dsel[j] = jnp.where(first, dirmat_ref[:, j, :], dirmat_ref[:, hloc + j, :])
    dmat = jnp.concatenate([dsel[j] for j in range(hloc)], axis=1)
    d1 = dmat.astype(bf16)
    rest = dmat - d1.astype(f32)
    d2 = rest.astype(bf16)
    d3 = (rest - d2.astype(f32)).astype(bf16)
    old_norm = jnp.sum(jnp.sum(res_ref[...] * res_ref[...], axis=0), keepdims=True)
    dir_norm = jnp.sum(jnp.sum(dir_ref[...] * dir_ref[...], axis=0), keepdims=True)
    mbuf[...] = jnp.full(mbuf.shape, -1e30, f32)

    def recv(buf, sem):
        rc(buf, buf, relay_send.at[0], sem, sib).wait_recv()

    recv(ain.at[other], sib_recv.at[0])
    recv(qin.at[other], sib_recv.at[1])
    recv(gin.at[other], sib_recv.at[2])
    recv(segbuf.at[SPAN + other], seg_recv.at[SPAN + other])
    recv(kbuf.at[SPAN + other], k_recv.at[SPAN + other])
    recv(vbuf.at[SPAN + other], v_recv.at[SPAN + other])

    for qb in range(2):
        a = ain[qb]
        lora = jnp.dot(a, up, preferred_element_type=f32)
        tan = (
            jnp.dot(a, d1, preferred_element_type=f32)
            + jnp.dot(a, d2, preferred_element_type=f32)
            + jnp.dot(a, d3, preferred_element_type=f32)
        ).astype(bf16)
        que = (qin[qb].astype(f32) + lora).astype(bf16)
        for j in range(hloc):
            h, g = j // per, j % per
            cols = slice(j * HEAD_DIM, (j + 1) * HEAD_DIM)
            rows = slice(g * tok, (g + 1) * tok)
            qs[qb, h, rows] = que[:, cols]
            ts[qb, h, rows] = tan[:, cols]
            gs[qb, h, rows] = gin[qb, :, cols]

    def stage(d):
        for s in range(2):
            w = SPAN - 2 * d + s
            seg_k = jnp.broadcast_to(segbuf[w], (tok, tok)).T
            for qb in range(2):
                if not qb <= w <= qb + SPAN:
                    continue
                allowed = seg_k == jnp.broadcast_to(segbuf[SPAN + qb], (tok, tok))
                if w == qb + SPAN:
                    allowed &= lax.broadcasted_iota(jnp.int32, (tok, tok), 0) <= lax.broadcasted_iota(
                        jnp.int32, (tok, tok), 1
                    )
                bias = jnp.where(allowed, 0.0, -1e30)
                for h in range(kvloc):
                    kb = kbuf[w, :, h * HEAD_DIM:(h + 1) * HEAD_DIM]
                    vb = vbuf[w, :, h * HEAD_DIM:(h + 1) * HEAD_DIM]
                    sc = lax.dot_general(kb, qs[qb, h], NT, preferred_element_type=f32)
                    for g in range(per):
                        cols = slice(g * tok, (g + 1) * tok)
                        part = sc[:, cols] + bias
                        sbuf[qb, h, w, :, cols] = part
                        top = jnp.max(part.reshape(tok // 8, 8, tok), axis=0)
                        mbuf[qb, h, :, cols] = jnp.maximum(mbuf[qb, h, :, cols], top)
                    tbuf[qb, h, w] = lax.dot_general(kb, ts[qb, h], NT, preferred_element_type=f32)
                    ubuf[qb, h, w] = lax.dot_general(vb, gs[qb, h], NT, preferred_element_type=f32)

    relay3, relay1 = [], []
    for s in range(2):
        w = SPAN - 4 + s
        n = 2 * (c - 1) + k
        relay1.append(rc(kbuf.at[w], kbuf.at[w + 2], relay_send.at[2 * s], k_recv.at[w + 2], n))
        relay1.append(rc(vbuf.at[w], vbuf.at[w + 2], relay_send.at[2 * s + 1], v_recv.at[w + 2], n))
    for s in range(2):
        w = SPAN - 2 + s
        n = 2 * (c + 2) + k
        relay3.append(rc(kbuf.at[w], kbuf.at[w - 4], relay_send.at[4 + 2 * s], k_recv.at[w - 4], n))
        relay3.append(rc(vbuf.at[w], vbuf.at[w - 4], relay_send.at[5 + 2 * s], v_recv.at[w - 4], n))

    def arrive(d, relays, cond):
        @pl.when(c >= d)
        def _():
            for s in range(2):
                w = SPAN - 2 * d + s
                recv(kbuf.at[w], k_recv.at[w])
                if relays:
                    pl.when(cond)(relays[2 * s].start)
                recv(vbuf.at[w], v_recv.at[w])
                if relays:
                    pl.when(cond)(relays[2 * s + 1].start)
            for s in range(2):
                w = SPAN - 2 * d + s
                recv(segbuf.at[w], seg_recv.at[w])

    stage(0)
    arrive(2, relay1, odd == 1)
    arrive(1, relay3, go2)
    stage(2)
    stage(1)
    arrive(3, [], None)
    stage(3)

    factor = HEAD_DIM ** -0.5 * 1.4426950408889634
    nblk = tok // 8
    for qb in range(2):
        at_ = ain[qb].astype(f32).T
        for h in range(kvloc):
            rows_of = []
            for g in range(per):
                cols = slice(g * tok, (g + 1) * tok)
                top = jnp.max(mbuf[qb, h, :, cols], axis=0, keepdims=True)

                def moments(w, acc, cols=cols, top=top, qb=qb, h=h):
                    e = jnp.exp2((sbuf[qb, h, qb + w, :, cols] - top) * factor)
                    sbuf[qb, h, qb + w, :, cols] = e
                    t = tbuf[qb, h, qb + w, :, cols]
                    u = ubuf[qb, h, qb + w, :, cols]
                    et = e * t

                    def fold(x):
                        return jnp.sum(x.reshape(nblk, 8, tok), axis=0)

                    return (acc[0] + fold(e), acc[1] + fold(et), acc[2] + fold(e * u), acc[3] + fold(et * u))

                zero = jnp.zeros((8, tok), f32)
                z, st, su, stu = lax.fori_loop(0, win, moments, (zero, zero, zero, zero))
                z, st, su, stu = (jnp.sum(x, axis=0, keepdims=True) for x in (z, st, su, stu))
                rz = 1.0 / z
                mt, mu = st * rz, su * rz
                cov = stu * rz - mt * mu

                def coefs(w, carry, cols=cols, mt=mt, mu=mu, cov=cov, qb=qb, h=h):
                    e = sbuf[qb, h, qb + w, :, cols]
                    t = tbuf[qb, h, qb + w, :, cols]
                    u = ubuf[qb, h, qb + w, :, cols]
                    cbuf[qb, h, w, :, cols] = (e * ((t - mt) * (u - mu) - cov)).astype(bf16)
                    return carry

                lax.fori_loop(0, win, coefs, 0)
                az = (at_ * rz).astype(bf16)
                cw = cbuf[qb, h, :, :, cols].reshape(win * tok, tok)
                rows_of.append(lax.dot_general(az, cw, NT, preferred_element_type=f32).astype(bf16))
            kw = kbuf[qb:qb + win, :, h * HEAD_DIM:(h + 1) * HEAD_DIM].reshape(win * tok, HEAD_DIM)
            hv = jnp.dot(jnp.concatenate(rows_of, axis=0), kw, preferred_element_type=f32)
            if qb == 0:
                hvacc[h] = hv
            else:
                hvacc[h] = (hvacc[h] + hv) * (1.0 / HEAD_DIM)

    dh = jnp.zeros((rank, LANES), f32)
    for j in range(hloc):
        h, g = j // per, j % per
        hv = hvacc[h, g * rank:(g + 1) * rank]
        hvsend[:, j // piece, j % piece, :] = hv
        dh = dh + hv * dsel[j]
    dh = jnp.sum(dh.reshape(rank // 8, 8, LANES), axis=0)
    dhsend[...] = dh
    dhrecv[me] = dh

    row0 = k * hloc
    groups = part_rows // piece

    def hv_copy(i):
        r, q = i // nq, lax.rem(i, nq)
        flat = r * heads + row0 + q * piece
        owner = flat // part_rows
        slot = c * groups + lax.rem(flat, part_rows) // piece
        return r, q, owner, slot, rc(hvsend.at[r, q], hvrecv.at[slot], hv_ssem.at[i], hv_rsem.at[slot], owner)

    def hv_start(i, carry):
        r, q, owner, slot, copy = hv_copy(i)
        pl.when(owner != me)(copy.start)

        @pl.when(owner == me)
        def _():
            hvrecv[slot] = hvsend[r, q]

        return carry

    lax.fori_loop(0, rank * nq, hv_start, 0)

    def dh_copy(i):
        return rc(dhsend, dhrecv.at[me], dh_ssem.at[i], dh_rsem.at[me], lax.rem(me + i, ctx))

    def each(lo, hi, body):
        def step(i, carry):
            body(i)
            return carry

        lax.fori_loop(lo, hi, step, 0)

    each(1, ctx, lambda i: dh_copy(i).start())

    my_q = me * part_rows // piece
    def hv_wait(slot):
        chip, grp = slot // groups, lax.rem(slot, groups)
        col = lax.rem(me * part_rows + grp * piece, heads)
        source = 2 * chip + col // hloc

        @pl.when(source != me)
        def _():
            recv(hvrecv.at[slot], hv_rsem.at[slot])

    each(0, chips * groups, hv_wait)

    def dh_wait(i):
        n = lax.rem(me + i, ctx)
        recv(dhrecv.at[n], dh_rsem.at[n])

    each(1, ctx, dh_wait)

    damp = damp_ref[0, 0]
    hv_sum = hvrecv[0:groups]
    for i in range(1, chips):
        hv_sum = hv_sum + hvrecv[i * groups:(i + 1) * groups]
    hv_sum = hv_sum.reshape(part_rows, LANES)
    dh_sum = jnp.sum(jnp.sum(dhrecv[...], axis=0), keepdims=True)
    step_len = old_norm / (dir_norm + dh_sum / damp)
    dir_part = dir_ref[me]
    curved = dir_part + hv_sum / damp
    nsol = sol_ref[me] + step_len * dir_part
    nres = res_ref[me] - step_len * curved
    nsol_ref[...] = nsol
    nres_ref[...] = nres
    sq = nres * nres
    tile = nrsend.shape[0]
    if part_rows > tile:
        sq = jnp.sum(sq.reshape(part_rows // tile, tile, LANES), axis=0)
    nrsend[...] = sq
    nrrecv[me] = sq
    solrecv[me_t] = nsol

    def nr_copy(i):
        return rc(nrsend, nrrecv.at[me], nr_ssem.at[i], nr_rsem.at[me], lax.rem(me + i, ctx))

    def sol_copy(i, slot):
        return pltpu.make_async_remote_copy(
            src_ref=nsol_ref, dst_ref=solrecv.at[slot], send_sem=sol_ssem.at[i], recv_sem=sol_rsem.at[slot],
            device_id=(lax.rem(me_t + i, tasks), me), device_id_type=MESH,
        )

    for i in range(1, tasks):
        sol_copy(i, me_t).start()
    each(1, ctx, lambda i: nr_copy(i).start())

    def drain(copies):
        for copy in copies:
            copy.wait_send()

    drain(sib_copies)
    pl.when(go2)(lambda: drain(ahead2))
    pl.when(go1)(lambda: drain(ahead1))
    for d, h, copy in seg_copies:
        ok = (c + d < chips) if d else (k != h)
        pl.when(ok)(copy.wait_send)
    pl.when((c >= 2) & (odd == 1))(lambda: drain(relay1))
    pl.when((c >= 1) & go2)(lambda: drain(relay3))

    def hv_drain(i):
        r, q, owner, slot, copy = hv_copy(i)
        pl.when(owner != me)(copy.wait_send)

    each(0, rank * nq, hv_drain)
    each(1, ctx, lambda i: dh_copy(i).wait_send())

    def nr_wait(i):
        n = lax.rem(me + i, ctx)
        recv(nrrecv.at[n], nr_rsem.at[n])

    each(1, ctx, nr_wait)
    ratio = jnp.sum(jnp.sum(nrrecv[...], axis=0), keepdims=True) / old_norm
    ndir_ref[...] = nres + ratio * dir_part
    for i in range(1, tasks):
        n = lax.rem(me_t + i, tasks)
        sol_copy(i, n).wait_recv()
    meta_ref[...] = jnp.sum(solrecv[...], axis=0) / tasks
    each(1, ctx, lambda i: nr_copy(i).wait_send())
    for i in range(1, tasks):
        sol_copy(i, me_t).wait_send()


def per_device(
    tasks, ctx,
    base_queries, adapter_input, adapter_up_weight, projected_keys, projected_values,
    output_gradient, segments, solution, residual, direction, damping,
):
    tok, features = base_queries.shape[1:]
    rank = adapter_input.shape[2]
    heads = features // HEAD_DIM
    params = direction.shape[1]
    part_rows = params // ctx // LANES
    hloc = heads // 2
    piece = min(part_rows, hloc)
    nq = hloc // piece
    chips = ctx // 2
    per = heads // KV_HEADS
    kvloc = KV_HEADS // 2
    khalf = projected_keys.shape[2] // 2
    half = features // 2
    nwin = SPAN + 2
    win = SPAN + 1
    slots = chips * (part_rows // piece)
    tile = min(8, part_rows)
    f32, bf16 = jnp.float32, jnp.bfloat16
    dma = pltpu.SemaphoreType.DMA
    vmem = pl.BlockSpec(memory_space=pltpu.VMEM)
    smem = pl.BlockSpec(memory_space=pltpu.SMEM)
    out = jax.ShapeDtypeStruct((part_rows, LANES), f32)
    dims = (tasks, ctx, rank, heads, part_rows, piece, nq)
    flat = (ctx, part_rows, LANES)
    stacked = (2, kvloc, nwin, tok, per * tok)
    outs = pl.pallas_call(
        functools.partial(kernel, dims),
        out_shape=[out] * 4,
        in_specs=[vmem] * 11 + [smem],
        out_specs=[vmem] * 4,
        scratch_shapes=[
            pltpu.VMEM((nwin, tok, khalf), bf16),
            pltpu.VMEM((nwin, tok, khalf), bf16),
            pltpu.VMEM((nwin, 1, tok), jnp.int32),
            pltpu.VMEM((2, tok, half), bf16),
            pltpu.VMEM((2, tok, half), bf16),
            pltpu.VMEM((2, tok, rank), bf16),
            pltpu.VMEM((2, kvloc, per * tok, HEAD_DIM), bf16),
            pltpu.VMEM((2, kvloc, per * tok, HEAD_DIM), bf16),
            pltpu.VMEM((2, kvloc, per * tok, HEAD_DIM), bf16),
            pltpu.VMEM((hloc, rank, LANES), f32),
            pltpu.VMEM(stacked, f32),
            pltpu.VMEM(stacked, f32),
            pltpu.VMEM(stacked, f32),
            pltpu.VMEM((2, kvloc, 8, per * tok), f32),
            pltpu.VMEM((2, kvloc, win, tok, per * tok), bf16),
            pltpu.VMEM((kvloc, per * rank, LANES), f32),
            pltpu.VMEM((rank, nq, piece, LANES), f32),
            pltpu.VMEM((slots, piece, LANES), f32),
            pltpu.VMEM((8, LANES), f32),
            pltpu.VMEM((ctx, 8, LANES), f32),
            pltpu.VMEM((tile, LANES), f32),
            pltpu.VMEM((ctx, tile, LANES), f32),
            pltpu.VMEM((tasks, part_rows, LANES), f32),
            dma((8,)), dma((5,)), dma((3,)), dma((8,)), dma((nwin,)), dma((nwin,)), dma((nwin,)), dma((8,)),
            dma((rank * nq,)), dma((slots,)), dma((ctx,)), dma((ctx,)), dma((ctx,)), dma((ctx,)),
            dma((tasks,)), dma((tasks,)),
        ],
        compiler_params=pltpu.CompilerParams(
            collective_id=0, has_side_effects=True, vmem_limit_bytes=60 * 1024 * 1024
        ),
    )(
        base_queries[0], adapter_input[0], adapter_up_weight[0], projected_keys[0], projected_values[0],
        output_gradient[0], segments, solution.reshape(flat), residual.reshape(flat), direction.reshape(flat),
        direction.reshape(rank, heads, LANES), damping.reshape(1, 1),
    )
    nsol, nres, ndir, meta = outs
    return nsol.reshape(1, -1), nres.reshape(1, -1), ndir.reshape(1, -1), meta.reshape(-1)


def solution(mesh):
    in_specs = (
        P("task", "ctx", None), P("task", "ctx", None), P("task", None, None), P("task", "ctx", None),
        P("task", "ctx", None), P("task", "ctx", None), P("task", "ctx"), P("task", None), P("task", None),
        P("task", None), P("task"),
    )
    out_specs = (P("task", "ctx"), P("task", "ctx"), P("task", "ctx"), P("ctx"))
    return jax.shard_map(
        functools.partial(per_device, mesh.shape["task"], mesh.shape["ctx"]),
        mesh=mesh, in_specs=in_specs, out_specs=out_specs, check_vma=False,
    )
```

```python
import functools

import jax
import jax.numpy as jnp
from jax import lax
from jax.experimental import pallas as pl
from jax.experimental.pallas import tpu as pltpu
from jax.sharding import PartitionSpec as P

KV_HEADS = 4
HEAD_DIM = 128
SPAN = 6
LANES = 128
MESH = pl.DeviceIdType.MESH
NT = (((1,), (1,)), ((), ()))


def kernel(
    dims,
    base_hbm, ain_ref, up_ref, key_hbm, val_hbm, grad_hbm, seg_ref,
    sol_ref, res_ref, dir_ref, dirmat_ref, damp_ref,
    nsol_ref, nres_ref, ndir_ref, meta_ref,
    base_ref, key_ref, val_ref, grad_ref, load_sem, tops, sums,
    kbuf, vbuf, segbuf, qin, gin, ain, qs, ts, gs, dsel,
    sbuf, tbuf, ubuf, mbuf, cbuf, hvacc, hvsend, hvrecv, dhsend, dhrecv,
    nrsend, nrrecv, solrecv,
    own_send, sib_send, sib_recv, seg_send, seg_recv, k_recv, v_recv, relay_send,
    hv_ssem, hv_rsem, dh_ssem, dh_rsem, nr_ssem, nr_rsem, sol_ssem, sol_rsem,
):
    tasks, ctx, rank, heads, part_rows, piece, nq = dims
    chips = ctx // 2
    per = heads // KV_HEADS
    tok = base_hbm.shape[0]
    half = heads * HEAD_DIM // 2
    khalf = key_hbm.shape[1] // 2
    hloc = heads // 2
    kvloc = KV_HEADS // 2
    nwin = SPAN + 2
    win = SPAN + 1
    back = SPAN // 2
    wide = per * tok
    f32, bf16 = jnp.float32, jnp.bfloat16
    me_t = lax.axis_index("task")
    me = lax.axis_index("ctx")
    c = me // 2
    k = lax.rem(me, 2)
    odd = lax.rem(c, 2)
    sib = me + 1 - 2 * k

    def dev(n):
        return (me_t, n)

    loads = [
        pltpu.make_async_copy(src, dst, load_sem.at[i])
        for i, (src, dst) in enumerate(
            ((key_hbm, key_ref), (val_hbm, val_ref), (base_hbm, base_ref), (grad_hbm, grad_ref))
        )
    ]
    for load in loads:
        load.start()
    barrier = pltpu.get_barrier_semaphore()

    def greet(i, carry):
        pl.semaphore_signal(barrier, inc=1, device_id=dev(lax.rem(me + i, ctx)), device_id_type=MESH)
        return carry

    lax.fori_loop(1, ctx, greet, 0)
    for i in range(1, tasks):
        pl.semaphore_signal(barrier, inc=1, device_id=(lax.rem(me_t + i, tasks), me), device_id_type=MESH)
    pl.semaphore_wait(barrier, ctx - 1 + tasks - 1)

    def rc(src, dst, ssem, rsem, n):
        return pltpu.make_async_remote_copy(
            src_ref=src, dst_ref=dst, send_sem=ssem, recv_sem=rsem, device_id=dev(n), device_id_type=MESH
        )

    def kcols(h):
        return pl.ds(pl.multiple_of(h * khalf, LANES), khalf)

    def qcols(h):
        return pl.ds(pl.multiple_of(h * half, LANES), half)

    other = 1 - k
    sib_copies = [
        rc(ain_ref, ain.at[k], sib_send.at[0], sib_recv.at[0], sib),
        rc(base_ref.at[:, qcols(other)], qin.at[k], sib_send.at[1], sib_recv.at[1], sib),
        rc(grad_ref.at[:, qcols(other)], gin.at[k], sib_send.at[2], sib_recv.at[2], sib),
        rc(key_ref.at[:, kcols(other)], kbuf.at[SPAN + k], sib_send.at[3], k_recv.at[SPAN + k], sib),
        rc(val_ref.at[:, kcols(other)], vbuf.at[SPAN + k], sib_send.at[4], v_recv.at[SPAN + k], sib),
    ]
    ahead2, ahead1 = [], []
    for h in range(2):
        for copies, d in ((ahead2, 2), (ahead1, 1)):
            n = 2 * (c + d) + h
            w = SPAN - 2 * d + k
            s = 4 * (d - 1) + 2 * h
            copies.append(rc(key_ref.at[:, kcols(h)], kbuf.at[w], own_send.at[s], k_recv.at[w], n))
            copies.append(rc(val_ref.at[:, kcols(h)], vbuf.at[w], own_send.at[s + 1], v_recv.at[w], n))
    seg_copies = []
    for d in range(back + 1):
        for h in range(2):
            w = SPAN - 2 * d + k
            n = 2 * (c + d) + h
            seg_copies.append((d, h, rc(seg_ref, segbuf.at[w], seg_send.at[2 * d + h], seg_recv.at[w], n)))
    go2 = c + 2 < chips
    go1 = odd == 0

    def start_all(copies):
        for copy in copies:
            copy.start()

    loads[0].wait()
    loads[1].wait()
    pl.when(go2)(lambda: start_all(ahead2))
    pl.when(go1)(lambda: start_all(ahead1))
    loads[2].wait()
    loads[3].wait()
    start_all(sib_copies)
    for d, h, copy in seg_copies:
        ok = (c + d < chips) if d else (k != h)
        pl.when(ok)(copy.start)

    for w in range(SPAN):
        @pl.when(c < back - w // 2)
        def _(w=w):
            kbuf[w] = jnp.zeros(kbuf.shape[1:], bf16)
            vbuf[w] = jnp.zeros(vbuf.shape[1:], bf16)
            segbuf[w] = jnp.full(segbuf.shape[1:], -1, jnp.int32)

    for s in range(2):
        @pl.when(k == s)
        def _(s=s):
            kbuf[SPAN + s] = key_ref[:, s * khalf:(s + 1) * khalf]
            vbuf[SPAN + s] = val_ref[:, s * khalf:(s + 1) * khalf]
            segbuf[SPAN + s] = seg_ref[...]
            qin[s] = base_ref[:, s * half:(s + 1) * half]
            gin[s] = grad_ref[:, s * half:(s + 1) * half]
            ain[s] = ain_ref[...]

    first = k == 0
    up = jnp.where(first, up_ref[:, :half].astype(f32), up_ref[:, half:].astype(f32)).astype(bf16)
    for j in range(hloc):
        dsel[j] = jnp.where(first, dirmat_ref[:, j, :], dirmat_ref[:, hloc + j, :])
    dmat = jnp.concatenate([dsel[j] for j in range(hloc)], axis=1)
    d1 = dmat.astype(bf16)
    rest = dmat - d1.astype(f32)
    d2 = rest.astype(bf16)
    d3 = (rest - d2.astype(f32)).astype(bf16)
    old_norm = jnp.sum(jnp.sum(res_ref[...] * res_ref[...], axis=0), keepdims=True)
    dir_norm = jnp.sum(jnp.sum(dir_ref[...] * dir_ref[...], axis=0), keepdims=True)
    mbuf[...] = jnp.full(mbuf.shape, -1e30, f32)

    def recv(buf, sem):
        rc(buf, buf, relay_send.at[0], sem, sib).wait_recv()

    recv(ain.at[other], sib_recv.at[0])
    recv(qin.at[other], sib_recv.at[1])
    recv(gin.at[other], sib_recv.at[2])
    recv(segbuf.at[SPAN + other], seg_recv.at[SPAN + other])
    recv(kbuf.at[SPAN + other], k_recv.at[SPAN + other])
    recv(vbuf.at[SPAN + other], v_recv.at[SPAN + other])

    for qb in range(2):
        a = ain[qb].astype(f32).T.astype(bf16)
        lora = jnp.dot(a, up, preferred_element_type=f32)
        tan = (
            jnp.dot(a, d1, preferred_element_type=f32)
            + jnp.dot(a, d2, preferred_element_type=f32)
            + jnp.dot(a, d3, preferred_element_type=f32)
        ).astype(bf16)
        que = (qin[qb].astype(f32) + lora).astype(bf16)
        for j in range(hloc):
            h, g = j // per, j % per
            cols = slice(j * HEAD_DIM, (j + 1) * HEAD_DIM)
            rows = slice(g * tok, (g + 1) * tok)
            qs[qb, h, rows] = que[:, cols]
            ts[qb, h, rows] = tan[:, cols]
            gs[qb, h, rows] = gin[qb, :, cols]

    def stage(d):
        for s in range(2):
            w = SPAN - 2 * d + s
            seg_k = jnp.broadcast_to(segbuf[w], (tok, tok)).T
            for qb in range(2):
                if not qb <= w <= qb + SPAN:
                    continue
                allowed = seg_k == jnp.broadcast_to(segbuf[SPAN + qb], (tok, tok))
                if w == qb + SPAN:
                    allowed &= lax.broadcasted_iota(jnp.int32, (tok, tok), 0) <= lax.broadcasted_iota(
                        jnp.int32, (tok, tok), 1
                    )
                bias = jnp.where(allowed, 0.0, -1e30)
                for h in range(kvloc):
                    kb = kbuf[w, :, h * HEAD_DIM:(h + 1) * HEAD_DIM]
                    vb = vbuf[w, :, h * HEAD_DIM:(h + 1) * HEAD_DIM]
                    sc = lax.dot_general(kb, qs[qb, h], NT, preferred_element_type=f32)
                    for g in range(per):
                        cols = slice(g * tok, (g + 1) * tok)
                        part = sc[:, cols] + bias
                        sbuf[qb, h, w, :, cols] = part
                        top = jnp.max(part.reshape(tok // 8, 8, tok), axis=0)
                        mbuf[qb, h, :, cols] = jnp.maximum(mbuf[qb, h, :, cols], top)
                    tbuf[qb, h, w] = lax.dot_general(kb, ts[qb, h], NT, preferred_element_type=f32)
                    ubuf[qb, h, w] = lax.dot_general(vb, gs[qb, h], NT, preferred_element_type=f32)

    factor = HEAD_DIM ** -0.5 * 1.4426950408889634
    nblk = tok // 8
    zero = jnp.zeros((8, tok), f32)

    def fold(x):
        return jnp.sum(x.reshape(nblk, 8, tok), axis=0)

    def moments(qb, h, w, cols, top, acc):
        e = jnp.exp2((sbuf[qb, h, w, :, cols] - top) * factor)
        sbuf[qb, h, w, :, cols] = e
        t = tbuf[qb, h, w, :, cols]
        u = ubuf[qb, h, w, :, cols]
        et = e * t
        return (acc[0] + fold(e), acc[1] + fold(et), acc[2] + fold(e * u), acc[3] + fold(et * u))

    def early_moments():
        for qb in range(2):
            for h in range(kvloc):
                for g in range(per):
                    cols = slice(g * tok, (g + 1) * tok)
                    top = jnp.max(mbuf[qb, h, :, cols], axis=0, keepdims=True)
                    tops[qb, h, :, cols] = jnp.broadcast_to(top, (8, tok))
                    acc = (zero,) * 4
                    for w in range(2, qb + win):
                        acc = moments(qb, h, w, cols, top, acc)
                    for i in range(4):
                        sums[qb, h, i, :, cols] = acc[i]

    relay3, relay1 = [], []
    for s in range(2):
        w = SPAN - 4 + s
        n = 2 * (c - 1) + k
        relay1.append(rc(kbuf.at[w], kbuf.at[w + 2], relay_send.at[2 * s], k_recv.at[w + 2], n))
        relay1.append(rc(vbuf.at[w], vbuf.at[w + 2], relay_send.at[2 * s + 1], v_recv.at[w + 2], n))
    for s in range(2):
        w = SPAN - 2 + s
        n = 2 * (c + 2) + k
        relay3.append(rc(kbuf.at[w], kbuf.at[w - 4], relay_send.at[4 + 2 * s], k_recv.at[w - 4], n))
        relay3.append(rc(vbuf.at[w], vbuf.at[w - 4], relay_send.at[5 + 2 * s], v_recv.at[w - 4], n))

    def arrive(d, relays, cond):
        @pl.when(c >= d)
        def _():
            for s in range(2):
                w = SPAN - 2 * d + s
                recv(kbuf.at[w], k_recv.at[w])
                if relays:
                    pl.when(cond)(relays[2 * s].start)
                recv(vbuf.at[w], v_recv.at[w])
                if relays:
                    pl.when(cond)(relays[2 * s + 1].start)
            for s in range(2):
                w = SPAN - 2 * d + s
                recv(segbuf.at[w], seg_recv.at[w])

    stage(0)
    arrive(2, relay1, odd == 1)
    arrive(1, relay3, go2)
    stage(2)
    stage(1)
    early_moments()
    arrive(3, [], None)
    stage(3)

    for qb in range(2):
        at_ = ain[qb].astype(f32)
        for h in range(kvloc):
            rows_of = []
            for g in range(per):
                cols = slice(g * tok, (g + 1) * tok)
                top = jnp.max(mbuf[qb, h, :, cols], axis=0, keepdims=True)
                shrink = jnp.exp2((tops[qb, h, 0:1, cols] - top) * factor)
                acc = tuple(sums[qb, h, i, :, cols] * shrink for i in range(4))
                for w in range(qb, 2):
                    acc = moments(qb, h, w, cols, top, acc)
                z, st, su, stu = (jnp.sum(x, axis=0, keepdims=True) for x in acc)
                rz = 1.0 / z
                mt, mu = st * rz, su * rz
                cov = stu * rz - mt * mu
                covs = cov * shrink
                for w in range(qb, qb + win):
                    e = sbuf[qb, h, w, :, cols]
                    t = tbuf[qb, h, w, :, cols] - mt
                    u = ubuf[qb, h, w, :, cols] - mu
                    inner = t * u - cov if w < 2 else t * (u * shrink) - covs
                    cbuf[qb, h, w - qb, :, cols] = (e * inner).astype(bf16)
                az = (at_ * rz).astype(bf16)
                blank = jnp.zeros(az.shape, bf16)
                rows_of.append(jnp.concatenate([az if i == g else blank for i in range(per)], axis=1))
            cw = cbuf[qb, h].reshape(win * tok, wide)
            gw = lax.dot_general(
                jnp.concatenate(rows_of, axis=0), cw, NT, preferred_element_type=f32
            ).astype(bf16)
            kw = kbuf[qb:qb + win, :, h * HEAD_DIM:(h + 1) * HEAD_DIM].reshape(win * tok, HEAD_DIM)
            hv = jnp.dot(gw, kw, preferred_element_type=f32)
            if qb == 0:
                hvacc[h] = hv
            else:
                hvacc[h] = (hvacc[h] + hv) * (1.0 / HEAD_DIM)

    dh = jnp.zeros((rank, LANES), f32)
    for j in range(hloc):
        h, g = j // per, j % per
        hv = hvacc[h, g * rank:(g + 1) * rank]
        hvsend[:, j // piece, j % piece, :] = hv
        dh = dh + hv * dsel[j]
    dh = jnp.sum(dh.reshape(rank // 8, 8, LANES), axis=0)
    dhsend[...] = dh
    dhrecv[me] = dh

    row0 = k * hloc
    groups = part_rows // piece

    def hv_copy(i):
        r, q = i // nq, lax.rem(i, nq)
        flat = r * heads + row0 + q * piece
        owner = flat // part_rows
        slot = c * groups + lax.rem(flat, part_rows) // piece
        return r, q, owner, slot, rc(hvsend.at[r, q], hvrecv.at[slot], hv_ssem.at[i], hv_rsem.at[slot], owner)

    def hv_start(i, carry):
        r, q, owner, slot, copy = hv_copy(i)
        pl.when(owner != me)(copy.start)

        @pl.when(owner == me)
        def _():
            hvrecv[slot] = hvsend[r, q]

        return carry

    lax.fori_loop(0, rank * nq, hv_start, 0)

    def dh_copy(i):
        return rc(dhsend, dhrecv.at[me], dh_ssem.at[i], dh_rsem.at[me], lax.rem(me + i, ctx))

    def each(lo, hi, body):
        def step(i, carry):
            body(i)
            return carry

        lax.fori_loop(lo, hi, step, 0)

    each(1, ctx, lambda i: dh_copy(i).start())

    my_q = me * part_rows // piece
    def hv_wait(slot):
        chip, grp = slot // groups, lax.rem(slot, groups)
        col = lax.rem(me * part_rows + grp * piece, heads)
        source = 2 * chip + col // hloc

        @pl.when(source != me)
        def _():
            recv(hvrecv.at[slot], hv_rsem.at[slot])

    each(0, chips * groups, hv_wait)

    def dh_wait(i):
        n = lax.rem(me + i, ctx)
        recv(dhrecv.at[n], dh_rsem.at[n])

    each(1, ctx, dh_wait)

    damp = damp_ref[0, 0]
    hv_sum = hvrecv[0:groups]
    for i in range(1, chips):
        hv_sum = hv_sum + hvrecv[i * groups:(i + 1) * groups]
    hv_sum = hv_sum.reshape(part_rows, LANES)
    dh_sum = jnp.sum(jnp.sum(dhrecv[...], axis=0), keepdims=True)
    step_len = old_norm / (dir_norm + dh_sum / damp)
    dir_part = dir_ref[me]
    curved = dir_part + hv_sum / damp
    nsol = sol_ref[me] + step_len * dir_part
    nres = res_ref[me] - step_len * curved
    nsol_ref[...] = nsol
    nres_ref[...] = nres
    sq = nres * nres
    tile = nrsend.shape[0]
    if part_rows > tile:
        sq = jnp.sum(sq.reshape(part_rows // tile, tile, LANES), axis=0)
    nrsend[...] = sq
    nrrecv[me] = sq
    solrecv[me_t] = nsol

    def nr_copy(i):
        return rc(nrsend, nrrecv.at[me], nr_ssem.at[i], nr_rsem.at[me], lax.rem(me + i, ctx))

    def sol_copy(i, slot):
        return pltpu.make_async_remote_copy(
            src_ref=nsol_ref, dst_ref=solrecv.at[slot], send_sem=sol_ssem.at[i], recv_sem=sol_rsem.at[slot],
            device_id=(lax.rem(me_t + i, tasks), me), device_id_type=MESH,
        )

    for i in range(1, tasks):
        sol_copy(i, me_t).start()
    each(1, ctx, lambda i: nr_copy(i).start())

    def drain(copies):
        for copy in copies:
            copy.wait_send()

    drain(sib_copies)
    pl.when(go2)(lambda: drain(ahead2))
    pl.when(go1)(lambda: drain(ahead1))
    for d, h, copy in seg_copies:
        ok = (c + d < chips) if d else (k != h)
        pl.when(ok)(copy.wait_send)
    pl.when((c >= 2) & (odd == 1))(lambda: drain(relay1))
    pl.when((c >= 1) & go2)(lambda: drain(relay3))

    def hv_drain(i):
        r, q, owner, slot, copy = hv_copy(i)
        pl.when(owner != me)(copy.wait_send)

    each(0, rank * nq, hv_drain)
    each(1, ctx, lambda i: dh_copy(i).wait_send())

    def nr_wait(i):
        n = lax.rem(me + i, ctx)
        recv(nrrecv.at[n], nr_rsem.at[n])

    each(1, ctx, nr_wait)
    ratio = jnp.sum(jnp.sum(nrrecv[...], axis=0), keepdims=True) / old_norm
    ndir_ref[...] = nres + ratio * dir_part
    for i in range(1, tasks):
        n = lax.rem(me_t + i, tasks)
        sol_copy(i, n).wait_recv()
    meta_ref[...] = jnp.sum(solrecv[...], axis=0) / tasks
    each(1, ctx, lambda i: nr_copy(i).wait_send())
    for i in range(1, tasks):
        sol_copy(i, me_t).wait_send()


def per_device(
    tasks, ctx,
    base_queries, adapter_input, adapter_up_weight, projected_keys, projected_values,
    output_gradient, segments, solution, residual, direction, damping,
):
    tok, features = base_queries.shape[1:]
    rank = adapter_input.shape[2]
    heads = features // HEAD_DIM
    params = direction.shape[1]
    part_rows = params // ctx // LANES
    hloc = heads // 2
    piece = min(part_rows, hloc)
    nq = hloc // piece
    chips = ctx // 2
    per = heads // KV_HEADS
    kvloc = KV_HEADS // 2
    khalf = projected_keys.shape[2] // 2
    half = features // 2
    nwin = SPAN + 2
    win = SPAN + 1
    slots = chips * (part_rows // piece)
    tile = min(8, part_rows)
    f32, bf16 = jnp.float32, jnp.bfloat16
    dma = pltpu.SemaphoreType.DMA
    vmem = pl.BlockSpec(memory_space=pltpu.VMEM)
    smem = pl.BlockSpec(memory_space=pltpu.SMEM)
    hbm = pl.BlockSpec(memory_space=pl.ANY)
    out = jax.ShapeDtypeStruct((part_rows, LANES), f32)
    dims = (tasks, ctx, rank, heads, part_rows, piece, nq)
    flat = (ctx, part_rows, LANES)
    stacked = (2, kvloc, nwin, tok, per * tok)
    outs = pl.pallas_call(
        functools.partial(kernel, dims),
        out_shape=[out] * 4,
        in_specs=[hbm, vmem, vmem, hbm, hbm, hbm] + [vmem] * 5 + [smem],
        out_specs=[vmem] * 4,
        scratch_shapes=[
            pltpu.VMEM((tok, features), bf16),
            pltpu.VMEM((tok, 2 * khalf), bf16),
            pltpu.VMEM((tok, 2 * khalf), bf16),
            pltpu.VMEM((tok, features), bf16),
            dma((4,)),
            pltpu.VMEM((2, kvloc, 8, per * tok), f32),
            pltpu.VMEM((2, kvloc, 4, 8, per * tok), f32),
            pltpu.VMEM((nwin, tok, khalf), bf16),
            pltpu.VMEM((nwin, tok, khalf), bf16),
            pltpu.VMEM((nwin, 1, tok), jnp.int32),
            pltpu.VMEM((2, tok, half), bf16),
            pltpu.VMEM((2, tok, half), bf16),
            pltpu.VMEM((2, rank, tok), bf16),
            pltpu.VMEM((2, kvloc, per * tok, HEAD_DIM), bf16),
            pltpu.VMEM((2, kvloc, per * tok, HEAD_DIM), bf16),
            pltpu.VMEM((2, kvloc, per * tok, HEAD_DIM), bf16),
            pltpu.VMEM((hloc, rank, LANES), f32),
            pltpu.VMEM(stacked, f32),
            pltpu.VMEM(stacked, f32),
            pltpu.VMEM(stacked, f32),
            pltpu.VMEM((2, kvloc, 8, per * tok), f32),
            pltpu.VMEM((2, kvloc, win, tok, per * tok), bf16),
            pltpu.VMEM((kvloc, per * rank, LANES), f32),
            pltpu.VMEM((rank, nq, piece, LANES), f32),
            pltpu.VMEM((slots, piece, LANES), f32),
            pltpu.VMEM((8, LANES), f32),
            pltpu.VMEM((ctx, 8, LANES), f32),
            pltpu.VMEM((tile, LANES), f32),
            pltpu.VMEM((ctx, tile, LANES), f32),
            pltpu.VMEM((tasks, part_rows, LANES), f32),
            dma((8,)), dma((5,)), dma((3,)), dma((8,)), dma((nwin,)), dma((nwin,)), dma((nwin,)), dma((8,)),
            dma((rank * nq,)), dma((slots,)), dma((ctx,)), dma((ctx,)), dma((ctx,)), dma((ctx,)),
            dma((tasks,)), dma((tasks,)),
        ],
        compiler_params=pltpu.CompilerParams(
            collective_id=0, has_side_effects=True, vmem_limit_bytes=60 * 1024 * 1024
        ),
    )(
        base_queries[0], adapter_input[0].T, adapter_up_weight[0], projected_keys[0], projected_values[0],
        output_gradient[0], segments, solution.reshape(flat), residual.reshape(flat), direction.reshape(flat),
        direction.reshape(rank, heads, LANES), damping.reshape(1, 1),
    )
    nsol, nres, ndir, meta = outs
    return nsol.reshape(1, -1), nres.reshape(1, -1), ndir.reshape(1, -1), meta.reshape(-1)


def solution(mesh):
    in_specs = (
        P("task", "ctx", None), P("task", "ctx", None), P("task", None, None), P("task", "ctx", None),
        P("task", "ctx", None), P("task", "ctx", None), P("task", "ctx"), P("task", None), P("task", None),
        P("task", None), P("task"),
    )
    out_specs = (P("task", "ctx"), P("task", "ctx"), P("task", "ctx"), P("ctx"))
    return jax.shard_map(
        functools.partial(per_device, mesh.shape["task"], mesh.shape["ctx"]),
        mesh=mesh, in_specs=in_specs, out_specs=out_specs, check_vma=False,
    )
```
